32 devices in a mesh: rep: 1, r: 8 (over y, z), s: 4 (over x, core).
Axes of the slice: x: 2, y: 2, z: 4, core: 2. Of those that a mesh axis runs over, the one named last changes fastest.
Arguments:
- x: bfloat16 [32, 4096, 512], P(('rep', 'r', 's'))
- dy: bfloat16 [32, 4096, 512], P(('rep', 'r', 's'))
- w_gate: bfloat16 [2, 512, 1408], P(None, 's')
- w_up: bfloat16 [2, 512, 1408], P(None, 's')
- w_down: bfloat16 [2, 1408, 512], P(None, 's')
- m_w_gate: float32 [2, 512, 1408], P(None, 's')
- m_w_up: float32 [2, 512, 1408], P(None, 's')
- m_w_down: float32 [2, 1408, 512], P(None, 's')
- v_w_gate: float32 [2, 512, 1408], P(None, 's')
- v_w_up: float32 [2, 512, 1408], P(None, 's')
- v_w_down: float32 [2, 1408, 512], P(None, 's')
Outputs:
- output 1: bfloat16 [2, 512, 1408], P('rep', 's')
- output 2: bfloat16 [2, 512, 1408], P('rep', 's')
- output 3: bfloat16 [2, 1408, 512], P('rep', 's')
- output 4: float32 [2, 512, 1408], P('rep', 's')
- output 5: float32 [2, 512, 1408], P('rep', 's')
- output 6: float32 [2, 1408, 512], P('rep', 's')
- output 7: float32 [2, 512, 1408], P('rep', 's')
- output 8: float32 [2, 512, 1408], P('rep', 's')
- output 9: float32 [2, 1408, 512], P('rep', 's')
All inputs are finite; a program needn't handle non-finite values.
Results may differ from the reference program's by a relative error of at most 0.022.
Values are sent between devices in bfloat16 or wider.
A program may use at most 2 GiB of HBM per device.

```python
import jax
import jax.numpy as jnp
from jax import lax

SEQUENCES = 32
TOKENS = 4096
D = 512
FF = 1408
LAYERS = 2
NAMES = ("w_gate", "w_up", "w_down")
SHAPES = {"w_gate": (LAYERS, D, FF), "w_up": (LAYERS, D, FF), "w_down": (LAYERS, FF, D)}


def bump(key, n, height):
    away = (jnp.arange(n, dtype=jnp.int32) - jax.random.randint(key, (), 0, n, jnp.int32)) % n
    return jnp.where(away < n // 8, height, 1.0)


def together(key, own, strength):
    shared = jax.random.normal(key, own.shape[1:], jnp.float32)
    return (own + strength * shared) * lax.rsqrt(1 + strength * strength)


def setup_inputs(seed: int = 0, part: int = 0) -> dict:
    kx, kdy, ka, kb, kz, kf, kh, kl, *keys = jax.random.split(jax.random.key(seed), 8 + 3 * len(NAMES))
    kx, kdy, ka, kb = (jax.random.fold_in(k, part) for k in (kx, kdy, ka, kb))
    kw, km, kv = (keys[i::3] for i in range(3))
    shape = (SEQUENCES, TOKENS, D)
    much_x, much_dy = jax.random.uniform(kz, (2,), jnp.float32, 0.0, 1.0)
    loud = 2.0 ** jax.random.uniform(jax.random.fold_in(kz, 1), (), jnp.float32, -1.0, 2.0)
    layers = 2.0 ** jax.random.uniform(kl, (LAYERS, 1, 1), jnp.float32, -1.0, 1.0)
    x = together(ka, jax.random.normal(kx, shape, jnp.float32), much_x) * bump(kf, D, 4.0)
    dy = together(kb, jax.random.normal(kdy, shape, jnp.float32), much_dy)
    drawn = {"x": x.astype(jnp.bfloat16), "dy": (loud * dy * (SEQUENCES * TOKENS) ** -0.5).astype(jnp.bfloat16)}
    for key, name in zip(kw, NAMES, strict=True):
        w = jax.random.normal(key, SHAPES[name], jnp.float32) * SHAPES[name][1] ** -0.5
        drawn[name] = (w * {"w_gate": 1.0, "w_up": bump(kh, FF, 4.0), "w_down": layers}[name]).astype(jnp.bfloat16)
    for key, name in zip(km, NAMES, strict=True):
        drawn[f"m_{name}"] = 0.1 * jax.random.normal(key, SHAPES[name], jnp.float32)
    for key, name in zip(kv, NAMES, strict=True):
        drawn[f"v_{name}"] = jax.random.uniform(key, SHAPES[name], jnp.float32, 0.005, 0.015)
    return drawn


def matmul(a, w):
    return jnp.dot(a, w, preferred_element_type=jnp.float32).astype(jnp.bfloat16)


def normed(h):
    wide = h.astype(jnp.float32)
    scale = lax.rsqrt(jnp.mean(wide**2, -1, keepdims=True) + 1e-6)
    return (wide * scale).astype(jnp.bfloat16)


def layer(h, w):
    a = normed(h)
    gate = jnp.dot(a, w["w_gate"], preferred_element_type=jnp.float32)
    up = jnp.dot(a, w["w_up"], preferred_element_type=jnp.float32)
    return h + matmul((jax.nn.silu(gate) * up).astype(jnp.bfloat16), w["w_down"])


def adamw(w, m, v, g):
    m = 0.9 * m + 0.1 * g
    v = 0.95 * v + 0.05 * g * g
    step = m * lax.rsqrt(v + 1e-8) + 0.1 * w
    return (w - 0.02 * step).astype(jnp.bfloat16), m, v


def clipped(gradients, sum_of_squares, count):
    factor = jnp.minimum(1.0, 0.5 * lax.rsqrt(sum_of_squares / count + 1e-30))
    return [g * factor for g in gradients]


def stack(weights, h):
    return lax.scan(lambda h, w: (layer(h, w), None), h, weights)[0]


def reference(x, dy, w_gate, w_up, w_down, m_w_gate, m_w_up, m_w_down, v_w_gate, v_w_up, v_w_down):
    weights = dict(zip(NAMES, (w_gate, w_up, w_down), strict=True))

    def take(so_far, sequence):
        h, by_y = sequence
        _, back = jax.vjp(lambda w: stack(w, h), weights)
        return jax.tree.map(lambda total, term: total + term.astype(jnp.float32), so_far, back(by_y)[0]), None

    none_yet = {name: jnp.zeros(w.shape, jnp.float32) for name, w in weights.items()}
    by_weights, _ = lax.scan(take, none_yet, (x, dy))
    gradients = [by_weights[name].astype(jnp.bfloat16).astype(jnp.float32) for name in NAMES]
    gradients = clipped(gradients, sum(jnp.sum(g * g) for g in gradients), sum(g.size for g in gradients))
    new = [
        adamw(w.astype(jnp.float32), m, v, g)
        for w, m, v, g in zip((w_gate, w_up, w_down), (m_w_gate, m_w_up, m_w_down), (v_w_gate, v_w_up, v_w_down), gradients, strict=True)
    ]
    return tuple(one[which] for which in range(3) for one in new)
```

```python
import functools

import jax
import jax.numpy as jnp
from jax import lax
from jax.experimental import pallas as pl
from jax.experimental.pallas import tpu as pltpu
from jax.sharding import PartitionSpec as P

F32, BF = jnp.float32, jnp.bfloat16
D, FF, TT = 512, 1408, 512
UNITS, SEG = 11, 32
ALL = 2 * UNITS
CHUNKS = ((0, 3), (3, 3), (6, 3), (9, 2))
COUNT = 2 * 3 * D * FF
VMEM_LIMIT = 62 * 2**20


def nn(a, b):
    return lax.dot_general(a, b, (((1,), (0,)), ((), ())), preferred_element_type=F32)


def nt(a, b):
    return lax.dot_general(a, b, (((1,), (1,)), ((), ())), preferred_element_type=F32)


def sigmoid(g):
    return 0.5 * jnp.tanh(0.5 * g) + 0.5


def backward_unit(g, u, d):
    s = sigmoid(g)
    silu = g * s
    return (silu * u).astype(BF), (d * u * (s + silu * (1.0 - s))).astype(BF), (d * silu).astype(BF)


def place():
    r, s = lax.axis_index("r"), lax.axis_index("s")
    return s // 2, s % 2, r // 4, r % 4


def device(x, core, y, z):
    return (0, y * 4 + z, x * 2 + core)


def remote(src, dst, send, recv, where):
    return pltpu.make_async_remote_copy(
        src_ref=src, dst_ref=dst, send_sem=send, recv_sem=recv, device_id=where, device_id_type=pl.DeviceIdType.MESH
    )


def greet(peers):
    barrier = pltpu.get_barrier_semaphore()
    for peer in peers:
        pl.semaphore_signal(barrier, inc=1, device_id=peer, device_id_type=pl.DeviceIdType.MESH)
    return lambda: pl.semaphore_wait(barrier, len(peers))


def pack(n, acc_gu, acc_d, row, out):
    for core in range(2):
        for x in range(2):
            s = 2 * x + core
            for p in range(8):
                y, z = p // 4, p % 4
                gu = pl.ds(pl.multiple_of(256 * row + 32 * p, 32), 32)
                d = pl.ds(pl.multiple_of(128 * row + SEG * s + 16 * y, 16), 16)
                out[n, core, x, p, 0:32, :] = acc_gu[gu, 128 * s : 128 * s + 128].astype(BF)
                out[n, core, x, p, 32:48, :] = acc_d[d, 128 * z : 128 * z + 128].astype(BF)


def first_kernel(
    x_ref, dy_ref, gate_ref, up_ref, down_ref, u_ref, dh_ref, wgu_out, wd_out,
    wgu, wd, h1s, act, dgu, wdt, wnat, acc_gu, acc_d, own_send, own_recv, send, recv, out_sem,
):
    i = pl.program_id(0)
    x, c, y, z = place()
    me, far = 2 * x + c, 2 * (1 - x) + c
    to_core, to_x, to_y = device(x, 1 - c, y, z), device(1 - x, c, y, z), device(x, c, 1 - y, z)

    def lanes(s):
        return pl.ds(pl.multiple_of(128 * s, 128), 128)

    def piece(l, p, s, half):
        if isinstance(p, int) and p == 4:
            return wd.at[l, :, s, pl.ds(pl.multiple_of(16 * half, 16), 16), :]
        return wgu.at[l, pl.ds(pl.multiple_of(1408 * half + 352 * p, 32), 352), lanes(s)]

    def copy(l, p, stage):
        half = 1 - y if stage == 3 else y
        ref = piece(l, p, me if stage == 0 else far, half)
        return remote(ref, ref, send.at[l, p, stage], recv.at[l, p, stage], (to_x, to_y, to_core, to_core)[stage])

    def own(l, k):
        ref = wd.at[l, :, me] if k else wgu.at[l, :, lanes(me)]
        return remote(ref, ref, own_send.at[l, k], own_recv.at[l, k], to_core)

    def out_copies():
        return (
            pltpu.make_async_copy(wgu.at[0], wgu_out, out_sem.at[0]),
            pltpu.make_async_copy(wd.at[0], wd_out, out_sem.at[1]),
        )

    def from_x(l, p):
        copy(l, p, 0).wait_recv()
        copy(l, p, 1).start()
        copy(l, p, 2).start()

    def from_y(l, p):
        copy(l, p, 1).wait_recv()
        copy(l, p, 3).start()

    def arrived(l):
        for k in range(2):
            own(l, k).wait_recv()
        for p in range(5):
            for stage in (2, 3):
                copy(l, p, stage).wait_recv()

    def place_own(l):
        for g, ref in enumerate((gate_ref, up_ref)):
            turned = ref[l].T
            for n in range(UNITS):
                for s in range(4):
                    wgu[l, 256 * n + 128 * g + SEG * s : 256 * n + 128 * g + SEG * s + SEG, lanes(me)] = turned[
                        352 * s + SEG * n : 352 * s + SEG * n + SEG, :
                    ]
        wd[l, :, me] = down_ref[l].reshape(UNITS, SEG, D)

    @pl.when(i == 0)
    def _():
        greeted = greet((to_core, to_x, to_y))
        place_own(0)
        greeted()
        for l in range(2):
            if l:
                place_own(1)
            for k in range(2):
                own(l, k).start()
            for p in range(5):
                copy(l, p, 0).start()
        for p in range(5):
            from_x(0, p)
            if p:
                from_y(0, p - 1)
        from_y(0, 4)
        acc_gu[...] = jnp.zeros_like(acc_gu)
        acc_d[...] = jnp.zeros_like(acc_d)
        arrived(0)
        wdt[...] = wd[0].reshape(FF, D).T
        for one in out_copies():
            one.start()

    @pl.when((i >= 1) & (i <= 4))
    def _():
        from_x(1, i - 1)

    @pl.when((i >= 2) & (i <= 5))
    def _():
        from_y(1, i - 2)

    @pl.when(i == 5)
    def _():
        from_x(1, 4)

    @pl.when(i == 6)
    def _():
        from_y(1, 4)

    @pl.when(i == 8)
    def _():
        arrived(1)
        wnat[...] = wgu[1].T

    @pl.when(i < 8)
    def _():
        x = x_ref[...]
        wide = x.astype(F32)
        a = (wide * lax.rsqrt(jnp.mean(wide * wide, -1, keepdims=True) + 1e-6)).astype(BF)
        for n in range(UNITS):
            gu = nt(wgu[0, 256 * n : 256 * n + 256, :], a)
            act[128 * n : 128 * n + 128, :] = (gu[:128] * sigmoid(gu[:128]) * gu[128:]).astype(BF)
        h1s[i] = (x.T.astype(F32) + nn(wdt[...], act[...]).astype(BF).astype(F32)).astype(BF)

    @pl.when(i >= 8)
    def _():
        wide = h1s[i - 8].astype(F32)
        scale = lax.rsqrt(jnp.mean(wide * wide, 0, keepdims=True) + 1e-6)
        a = (wide * scale).astype(BF)
        dy = dy_ref[...]
        for n in range(UNITS):
            gu = nn(wgu[1, 256 * n : 256 * n + 256, :], a)
            d = nt(wd[1, n].reshape(128, D), dy).astype(BF).astype(F32)
            one, dg, du = backward_unit(gu[:128], gu[128:], d)
            act[128 * n : 128 * n + 128, :] = one
            dgu[256 * n : 256 * n + 128, :] = dg
            dgu[256 * n + 128 : 256 * n + 256, :] = du
        acc_d[...] += nn(act[...], dy)
        acc_gu[...] += nt(dgu[...], a)
        da = nn(wnat[...], dgu[...]).astype(BF).astype(F32)
        back = scale * da - wide * (scale * scale * scale * jnp.mean(wide * da, 0, keepdims=True))
        dh_ref[0] = (dy.T.astype(F32) + back.astype(BF).astype(F32)).astype(BF)

    @pl.when(i == 15)
    def _():
        @pl.loop(0, UNITS)
        def _(n):
            pack(n, acc_gu, acc_d, n, u_ref)

        for one in out_copies():
            one.wait()
        for l in range(2):
            for k in range(2):
                own(l, k).wait_send()
            for p in range(5):
                for stage in range(4):
                    copy(l, p, stage).wait_send()


def second_kernel(
    x_any, dh_any, wgu_any, wd_any, u_any, g_out, total_out,
    xs, a0, dh, wgu, wd, u, gu_s, d_s, act, dgu, acc_gu, acc_d,
    rc, sx, rx, sy, ry, sz, rz, g, sums, squares,
    s1, r1, s3, r3, norm_send, norm_recv, in_sem, tile_sem, out_sem,
):
    x, c, y, z = place()
    to_core, to_x, to_y = device(x, 1 - c, y, z), device(1 - x, c, y, z), device(x, c, 1 - y, z)
    to_z = [device(x, c, y, (z + k) % 4) for k in (1, 2, 3)]
    group = [to_core, to_x, device(1 - x, 1 - c, y, z)]
    greeted = greet([to_core, to_x, to_y, *to_z, group[2]])

    loads = [
        pltpu.make_async_copy(wgu_any, wgu, in_sem.at[0]),
        pltpu.make_async_copy(wd_any, wd, in_sem.at[1]),
        pltpu.make_async_copy(u_any, u.at[pl.ds(0, UNITS)], in_sem.at[2]),
    ]

    def tile_loads(t):
        rows = pl.ds(pl.multiple_of(TT * t, TT), TT)
        return pltpu.make_async_copy(x_any.at[rows], xs.at[t], tile_sem.at[t, 0]), pltpu.make_async_copy(dh_any.at[t], dh.at[t], tile_sem.at[t, 1])

    loads[0].start()
    for t in range(8):
        for one in tile_loads(t):
            one.start()
        if t == 0:
            loads[1].start()
            loads[2].start()
    squares[...] = jnp.zeros_like(squares)

    def c_copy(q):
        return remote(u.at[q, 1 - c], rc.at[q], s1.at[q, 0], r1.at[q, 0], to_core)

    def x_copy(q):
        return remote(sx.at[q], rx.at[q], s1.at[q, 1], r1.at[q, 1], to_x)

    def y_copy(q):
        return remote(sy.at[q], ry.at[q], s1.at[q, 2], r1.at[q, 2], to_y)

    def z_copy(q, k):
        return remote(sz.at[q, k], rz.at[q, k], s3.at[q, 0, k], r3.at[q, 0, k], to_z[k])

    def back_z_copy(q, k):
        return remote(g.at[q, 4 * y + z], g.at[q, 4 * y + z], s3.at[q, 1, k], r3.at[q, 1, k], to_z[k])

    def back_y_copy(q):
        half = g.at[q, pl.ds(4 * y, 4)]
        return remote(half, half, s1.at[q, 3], r1.at[q, 3], to_y)

    def upto_x(q, p):
        return u[q, c, x, p].astype(F32) + rc[q, x, p].astype(F32) + rx[q, p].astype(F32)

    def upto_y(q, k):
        return upto_x(q, 4 * y + k) + ry[q, k].astype(F32)

    def stage0(q):
        c_copy(q).start()

    def stage1(q):
        c_copy(q).wait_recv()
        sx[q] = (u[q, c, 1 - x].astype(F32) + rc[q, 1 - x].astype(F32)).astype(BF)
        x_copy(q).start()

    def stage2(q):
        x_copy(q).wait_recv()
        for k in range(4):
            sy[q, k] = upto_x(q, 4 * (1 - y) + k).astype(BF)
        y_copy(q).start()

    def stage3(q):
        y_copy(q).wait_recv()
        for k in range(3):
            sz[q, k] = upto_y(q, (z + k + 1) % 4).astype(BF)
        for k in range(3):
            z_copy(q, k).start()

    def stage4(q):
        for k in range(3):
            z_copy(q, k).wait_recv()
        total = upto_y(q, z)
        for k in range(3):
            total += rz[q, k].astype(F32)
        g[q, 4 * y + z] = total.astype(BF)
        for k in range(3):
            back_z_copy(q, k).start()

    def stage5(q):
        for k in range(3):
            back_z_copy(q, k).wait_recv()
        back_y_copy(q).start()

    def stage6(q):
        back_y_copy(q).wait_recv()
        wide = g[q].astype(F32).reshape(48, 8, 128)
        squares[...] += jnp.sum(wide * wide, 0)

    stages = (stage0, stage1, stage2, stage3, stage4, stage5, stage6)

    def tick(m):
        for j in reversed(range(7)):
            q = m - 2 * j

            @pl.when((q >= 0) & (q < ALL))
            def _():
                stages[j](q)

    for number, (first, units) in enumerate(CHUNKS):
        if number == 0:
            loads[0].wait()
            loads[1].wait()

        @pl.loop(0, 8)
        def _(t):
            if number == 0:
                for one in tile_loads(t):
                    one.wait()
                wide = xs[t].astype(F32)
                a0[t] = (wide * lax.rsqrt(jnp.mean(wide * wide, -1, keepdims=True) + 1e-6)).astype(BF)
            gu_s[: 256 * units, :] = nt(wgu[256 * first : 256 * (first + units), :], a0[t])
            d_s[: 128 * units, :] = nn(wd[first : first + units].reshape(128 * units, D), dh[t])
            for n in range(units):
                low = 256 * n
                one, dg, du = backward_unit(
                    gu_s[low : low + 128, :], gu_s[low + 128 : low + 256, :], d_s[128 * n : 128 * n + 128, :].astype(BF).astype(F32)
                )
                act[128 * n : 128 * n + 128, :] = one
                dgu[low : low + 128, :] = dg
                dgu[low + 128 : low + 256, :] = du
            new_d = nt(act[: 128 * units, :], dh[t])
            new_gu = nn(dgu[: 256 * units, :], a0[t])

            @pl.when(t == 0)
            def _():
                acc_d[: 128 * units, :] = new_d
                acc_gu[: 256 * units, :] = new_gu

            @pl.when(t > 0)
            def _():
                acc_d[: 128 * units, :] += new_d
                acc_gu[: 256 * units, :] += new_gu

            if number == 0:

                @pl.when(t == 1)
                def _():
                    greeted()
                    loads[2].wait()

            @pl.when(t % 2 == 1)
            def _():
                tick(4 * number + t // 2)

        @pl.loop(0, units)
        def _(n):
            pack(UNITS + first + n, acc_gu, acc_d, n, u)

    @pl.loop(16, ALL + 12)
    def _(m):
        tick(m)

    mine = sums.at[2 * x + c]
    norm = [remote(mine, mine, norm_send.at[k], norm_recv.at[k], group[k]) for k in range(3)]
    sums[2 * x + c] = squares[...]
    for one in norm:
        one.start()
    out = pltpu.make_async_copy(g, g_out, out_sem.at[0])
    out.start()

    @pl.loop(0, ALL)
    def _(q):
        for one in (c_copy(q), x_copy(q), y_copy(q), back_y_copy(q)):
            one.wait_send()
        for k in range(3):
            z_copy(q, k).wait_send()
            back_z_copy(q, k).wait_send()

    for one in norm:
        one.wait()
    total_out[...] = sums[0] + sums[1] + sums[2] + sums[3]
    out.wait()


def third_kernel(g_ref, total_ref, *refs):
    weights, ms, vs = refs[0:3], refs[3:6], refs[6:9]
    new_w, new_m, new_v = refs[9:12], refs[12:15], refs[15:18]
    turned, plain = refs[18:20]
    factor = jnp.minimum(1.0, 0.5 * lax.rsqrt(jnp.sum(total_ref[...]) / COUNT + 1e-30))

    def take(i, g):
        g = g * factor
        m = 0.9 * ms[i][0] + 0.1 * g
        v = 0.95 * vs[i][0] + 0.05 * g * g
        w = weights[i][0].astype(F32)
        new_m[i][0] = m
        new_v[i][0] = v
        new_w[i][0] = (w - 0.02 * (m * lax.rsqrt(v + 1e-8) + 0.1 * w)).astype(BF)

    for i in range(2):
        for n in range(UNITS):
            for s in range(4):
                turned[352 * s + SEG * n : 352 * s + SEG * n + SEG, :] = g_ref[0, n, 4 * i + s, 0:32, :].astype(F32)
        take(i, turned[...].T)
    for n in range(UNITS):
        for p in range(8):
            row = SEG * n + 16 * (p // 4)
            plain[row : row + 16, 128 * (p % 4) : 128 * (p % 4) + 128] = g_ref[0, n, p, 32:48, :].astype(F32)
    take(2, plain[...])


def step(x, dy, w_gate, w_up, w_down, *moments):
    tokens = x.shape[1]
    tiles = tokens // TT
    any_ = pl.BlockSpec(memory_space=pl.ANY)

    def once(shape):
        return pl.BlockSpec(shape, lambda i: (0,) * len(shape), pipeline_mode=pl.Buffered(1))

    unit = (UNITS, 2, 2, 8, 48, 128)
    dma = pltpu.SemaphoreType.DMA
    u1, dh, wgu0, wd0 = pl.pallas_call(
        first_kernel,
        grid=(2 * tiles,),
        in_specs=[
            pl.BlockSpec((TT, D), lambda i: (jnp.minimum(i, tiles - 1), 0)),
            pl.BlockSpec((TT, D), lambda i: (jnp.maximum(i - tiles, 0), 0)),
            once(w_gate.shape), once(w_up.shape), once(w_down.shape),
        ],
        out_specs=[once(unit), pl.BlockSpec((1, D, TT), lambda i: (jnp.maximum(i - tiles, 0), 0, 0)), any_, any_],
        out_shape=[
            jax.ShapeDtypeStruct(unit, BF),
            jax.ShapeDtypeStruct((tiles, D, TT), BF),
            jax.ShapeDtypeStruct((2 * FF, D), BF),
            jax.ShapeDtypeStruct((UNITS, 4, SEG, D), BF),
        ],
        scratch_shapes=[
            pltpu.VMEM((2, 2 * FF, D), BF),
            pltpu.VMEM((2, UNITS, 4, SEG, D), BF),
            pltpu.VMEM((tiles, D, TT), BF),
            pltpu.VMEM((FF, TT), BF),
            pltpu.VMEM((2 * FF, TT), BF),
            pltpu.VMEM((D, FF), BF),
            pltpu.VMEM((D, 2 * FF), BF),
            pltpu.VMEM((2 * FF, D), F32),
            pltpu.VMEM((FF, D), F32),
            dma((2, 2)), dma((2, 2)), dma((2, 5, 4)), dma((2, 5, 4)), dma((2,)),
        ],
        compiler_params=pltpu.CompilerParams(vmem_limit_bytes=VMEM_LIMIT, collective_id=0, has_side_effects=True),
        name="gather_forward_and_last_layer",
    )(x[0], dy[0], w_gate, w_up, w_down)

    most = max(units for _, units in CHUNKS)
    g, total = pl.pallas_call(
        second_kernel,
        in_specs=[any_] * 5,
        out_specs=[any_, pl.BlockSpec(memory_space=pltpu.VMEM)],
        out_shape=[jax.ShapeDtypeStruct((ALL, 8, 48, 128), BF), jax.ShapeDtypeStruct((8, 128), F32)],
        scratch_shapes=[
            pltpu.VMEM((tiles, TT, D), BF),
            pltpu.VMEM((tiles, TT, D), BF),
            pltpu.VMEM((tiles, D, TT), BF),
            pltpu.VMEM((2 * FF, D), BF),
            pltpu.VMEM((UNITS, 4, SEG, D), BF),
            pltpu.VMEM((ALL, 2, 2, 8, 48, 128), BF),
            pltpu.VMEM((256 * most, TT), F32),
            pltpu.VMEM((128 * most, TT), F32),
            pltpu.VMEM((128 * most, TT), BF),
            pltpu.VMEM((256 * most, TT), BF),
            pltpu.VMEM((256 * most, D), F32),
            pltpu.VMEM((128 * most, D), F32),
            pltpu.VMEM((ALL, 2, 8, 48, 128), BF),
            pltpu.VMEM((ALL, 8, 48, 128), BF),
            pltpu.VMEM((ALL, 8, 48, 128), BF),
            pltpu.VMEM((ALL, 4, 48, 128), BF),
            pltpu.VMEM((ALL, 4, 48, 128), BF),
            pltpu.VMEM((ALL, 3, 48, 128), BF),
            pltpu.VMEM((ALL, 3, 48, 128), BF),
            pltpu.VMEM((ALL, 8, 48, 128), BF),
            pltpu.VMEM((4, 8, 128), F32),
            pltpu.VMEM((8, 128), F32),
            dma((ALL, 4)), dma((ALL, 4)), dma((ALL, 2, 3)), dma((ALL, 2, 3)),
            dma((3,)), dma((3,)), dma((3,)), dma((tiles, 2)), dma((1,)),
        ],
        compiler_params=pltpu.CompilerParams(vmem_limit_bytes=VMEM_LIMIT, collective_id=1, has_side_effects=True),
        name="first_layer_and_sums",
    )(x[0], dh, wgu0, wd0, u1)

    arrays = (w_gate, w_up, w_down, *moments)

    def by_layer(a):
        return pl.BlockSpec((1,) + a.shape[1:], lambda l: (l, 0, 0))

    return pl.pallas_call(
        third_kernel,
        grid=(2,),
        in_specs=[pl.BlockSpec((1, UNITS, 8, 48, 128), lambda l: (1 - l, 0, 0, 0, 0)), pl.BlockSpec((8, 128), lambda l: (0, 0))]
        + [by_layer(a) for a in arrays],
        out_specs=[by_layer(a) for a in arrays],
        out_shape=[jax.ShapeDtypeStruct(a.shape, a.dtype) for a in arrays],
        scratch_shapes=[pltpu.VMEM((FF, 128), F32), pltpu.VMEM((FF // 4, D), F32)],
        compiler_params=pltpu.CompilerParams(vmem_limit_bytes=VMEM_LIMIT),
        name="clip_and_adamw",
    )(g.reshape(2, UNITS, 8, 48, 128), total, *arrays)


def solution(mesh):
    states, cut = P(("rep", "r", "s"), None, None), P(None, "s", None)
    return jax.shard_map(
        lambda *arrays: tuple(step(*arrays)),
        mesh=mesh,
        in_specs=(states, states) + (cut,) * 9,
        out_specs=(P("rep", "s", None),) * 9,
        check_vma=False,
    )
```

```python
import functools

import jax
import jax.numpy as jnp
from jax import lax
from jax.experimental import pallas as pl
from jax.experimental.pallas import tpu as pltpu
from jax.sharding import PartitionSpec as P

F32, BF = jnp.float32, jnp.bfloat16
D, FF, TT, WIDE = 512, 1408, 512, 1024
UNITS, SEG = 11, 32
ALL = 2 * UNITS
CHUNKS = ((0, 3), (3, 3), (6, 3), (9, 2))
COUNT = 2 * 3 * D * FF
MIB = 2**20
VMEM_LIMIT = 62 * MIB
LANE, PAIR = 128, 256


def nn(a, b):
    return lax.dot_general(a, b, (((1,), (0,)), ((), ())), preferred_element_type=F32)


def nt(a, b):
    return lax.dot_general(a, b, (((1,), (1,)), ((), ())), preferred_element_type=F32)


def sigmoid(g):
    return 0.5 * jnp.tanh(0.5 * g) + 0.5


def backward_unit(g, u, d):
    s = sigmoid(g)
    silu = g * s
    return (silu * u).astype(BF), (d * u * (s + silu * (1.0 - s))).astype(BF), (d * silu).astype(BF)


def place():
    r, s = lax.axis_index("r"), lax.axis_index("s")
    return s // 2, s % 2, r // 4, r % 4


def device(x, core, y, z):
    return (0, y * 4 + z, x * 2 + core)


def remote(src, dst, send, recv, where):
    return pltpu.make_async_remote_copy(
        src_ref=src, dst_ref=dst, send_sem=send, recv_sem=recv, device_id=where, device_id_type=pl.DeviceIdType.MESH
    )


def greet(peers):
    barrier = pltpu.get_barrier_semaphore()
    for peer in peers:
        pl.semaphore_signal(barrier, inc=1, device_id=peer, device_id_type=pl.DeviceIdType.MESH)
    return lambda: pl.semaphore_wait(barrier, len(peers))


def pack(n, acc_gu, acc_d, row, out):
    for core in range(2):
        for x in range(2):
            s = 2 * x + core
            for p in range(8):
                y, z = p // 4, p % 4
                gu = pl.ds(pl.multiple_of(PAIR * row + 32 * p, 32), 32)
                d = pl.ds(pl.multiple_of(LANE * row + SEG * s + 16 * y, 16), 16)
                out[n, core, x, p, 0:32, :] = acc_gu[gu, LANE * s : LANE * s + LANE].astype(BF)
                out[n, core, x, p, 32:48, :] = acc_d[d, LANE * z : LANE * z + LANE].astype(BF)


def first_kernel(
    x_ref, dy_ref, gate_ref, up_ref, down_ref, u_ref, dh_ref, gu_out, wd_out,
    wgu, wd, h1s, acts, a_first, stage, dgu, wdt, acc_gu, acc_d, own_send, own_recv, send, recv, gu_sem, out_sem,
):
    i = pl.program_id(0)
    x, c, y, z = place()
    me, far = 2 * x + c, 2 * (1 - x) + c
    to_core, to_x, to_y = device(x, 1 - c, y, z), device(1 - x, c, y, z), device(x, c, 1 - y, z)

    def lanes(s):
        return pl.ds(pl.multiple_of(LANE * s, LANE), LANE)

    def piece(l, p, s, half):
        if p == 4:
            return wd.at[l, :, s, pl.ds(pl.multiple_of(16 * half, 16), 16), :]
        first, units = CHUNKS[p]
        return wgu.at[l, pl.ds(first, units), half, :, lanes(s)]

    def copy(l, p, stage):
        half = 1 - y if stage == 3 else y
        ref = piece(l, p, me if stage == 0 else far, half)
        return remote(ref, ref, send.at[l, p, stage], recv.at[l, p, stage], (to_x, to_y, to_core, to_core)[stage])

    def own(l, k):
        ref = wd.at[l, :, me] if k else wgu.at[l, :, :, :, lanes(me)]
        return remote(ref, ref, own_send.at[l, k], own_recv.at[l, k], to_core)

    wd_copy = pltpu.make_async_copy(wd, wd_out, out_sem.at[0])

    def gu_copy(p, t):
        first, units = CHUNKS[p]
        rows = pl.ds(first, units)
        there = gu_out.at[rows, t // 2, :, pl.ds(pl.multiple_of(TT * (t % 2), TT), TT)]
        return pltpu.make_async_copy(stage.at[t % 2, rows], there, gu_sem.at[p, t % 2])

    def from_x(l, p):
        copy(l, p, 0).wait_recv()
        copy(l, p, 1).start()
        copy(l, p, 2).start()

    def from_y(l, p):
        copy(l, p, 1).wait_recv()
        copy(l, p, 3).start()

    def arrived(l, p):
        for stage in (2, 3):
            copy(l, p, stage).wait_recv()

    def place_own(l):
        for g, ref in enumerate((gate_ref, up_ref)):
            turned = ref[l].T
            for n in range(UNITS):
                for s in range(4):
                    wgu[l, n, g, SEG * s : SEG * s + SEG, lanes(me)] = turned[
                        352 * s + SEG * n : 352 * s + SEG * n + SEG, :
                    ]
        wd[l, :, me] = down_ref[l].reshape(UNITS, SEG, D)

    def up_and_gate(first, units, a, out, slot):
        for n in range(first, first + units):
            gu = nt(wgu[0, n].reshape(PAIR, D), a)
            stage[slot, n] = gu
            out[LANE * n : LANE * n + LANE, :] = (gu[:LANE] * sigmoid(gu[:LANE]) * gu[LANE:]).astype(BF)

    def down(x, act, t):
        h1s[t] = (x.T.astype(F32) + nn(wdt[...], act[...]).astype(BF).astype(F32)).astype(BF)

    @pl.when(i == 0)
    def _():
        greeted = greet((to_core, to_x, to_y))
        place_own(0)
        greeted()
        for l in range(2):
            if l:
                place_own(1)
            for k in range(2):
                own(l, k).start()
            for p in range(5):
                copy(l, p, 0).start()
        acc_gu[...] = jnp.zeros_like(acc_gu)
        acc_d[...] = jnp.zeros_like(acc_d)
        own(0, 0).wait_recv()
        from_x(0, 0)
        for p in range(4):
            from_x(0, p + 1)
            from_y(0, p)
            arrived(0, p)
            first, units = CHUNKS[p]

            @pl.loop(0, 4)
            def _(t):
                if p == 0:
                    wide = x_ref[t].astype(F32)
                    a_first[t] = (wide * lax.rsqrt(jnp.mean(wide * wide, -1, keepdims=True) + 1e-6)).astype(BF)

                @pl.when(t >= 2)
                def _():
                    gu_copy(p, t - 2).wait()

                up_and_gate(first, units, a_first[t], acts.at[t], t % 2)
                gu_copy(p, t).start()

        from_y(0, 4)
        own(0, 1).wait_recv()
        arrived(0, 4)
        wdt[...] = wd[0].reshape(FF, D).T

        @pl.loop(0, 4)
        def _(t):
            for p in range(4):

                @pl.when(t == p)
                def _():
                    from_x(1, p)

            down(x_ref[t], acts.at[t], t)

    @pl.when(i == 1)
    def _():
        @pl.loop(0, 4)
        def _(t):
            @pl.when(t == 0)
            def _():
                from_y(1, 0)
                from_y(1, 1)

            @pl.when(t == 1)
            def _():
                from_x(1, 4)
                from_y(1, 2)

            @pl.when(t == 2)
            def _():
                from_y(1, 3)

            @pl.when(t == 3)
            def _():
                from_y(1, 4)

            x = x_ref[t]
            wide = x.astype(F32)
            a = (wide * lax.rsqrt(jnp.mean(wide * wide, -1, keepdims=True) + 1e-6)).astype(BF)
            for p in range(4):
                gu_copy(p, t + 2).wait()
            up_and_gate(0, UNITS, a, acts.at[0], t % 2)
            for p in range(4):
                gu_copy(p, t + 4).start()
            down(x, acts.at[0], 4 + t)

        for k in range(2):
            own(1, k).wait_recv()
        for p in range(5):
            arrived(1, p)
        wd_copy.start()

    @pl.when(i >= 2)
    def _():
        act = acts.at[0]
        wide = h1s[i - 2].astype(F32)
        scale = lax.rsqrt(jnp.mean(wide * wide, 0, keepdims=True) + 1e-6)
        a = (wide * scale).astype(BF)
        dy = dy_ref[...]
        dyt = dy.T
        for n in range(UNITS):
            gu = nn(wgu[1, n].reshape(PAIR, D), a)
            d = nn(wd[1, n].reshape(LANE, D), dyt).astype(BF).astype(F32)
            one, dg, du = backward_unit(gu[:LANE], gu[LANE:], d)
            act[LANE * n : LANE * n + LANE, :] = one
            dgu[PAIR * n : PAIR * n + LANE, :] = dg
            dgu[PAIR * n + LANE : PAIR * n + PAIR, :] = du
        acc_d[...] += nn(act[...], dy)
        acc_gu[...] += nt(dgu[...], a)
        da = lax.dot_general(wgu[1].reshape(2 * FF, D), dgu[...], (((0,), (0,)), ((), ())), preferred_element_type=F32).astype(BF).astype(F32)
        back = scale * da - wide * (scale * scale * scale * jnp.mean(wide * da, 0, keepdims=True))
        dh_ref[0] = (dyt.astype(F32) + back.astype(BF).astype(F32)).astype(BF)

    @pl.when(i == 9)
    def _():
        @pl.loop(0, UNITS)
        def _(n):
            pack(n, acc_gu, acc_d, n, u_ref)

        wd_copy.wait()
        for p in range(4):
            for t in (6, 7):
                gu_copy(p, t).wait()
        for l in range(2):
            for k in range(2):
                own(l, k).wait_send()
            for p in range(5):
                for stage in range(4):
                    copy(l, p, stage).wait_send()


def second_kernel(
    x_any, dh_any, gu_any, wd_any, u_any, g_out, total_out,
    a0, dh, gu, wd, u, act, dgu, acc_gu, acc_d,
    rc, sx, rx, sy, ry, sz, rz, g, sums, squares,
    s1, r1, s3, r3, norm_send, norm_recv, in_sem, tile_sem,
):
    x, c, y, z = place()
    to_core, to_x, to_y = device(x, 1 - c, y, z), device(1 - x, c, y, z), device(x, c, 1 - y, z)
    to_z = [device(x, c, y, (z + k) % 4) for k in (1, 2, 3)]
    group = [to_core, to_x, device(1 - x, 1 - c, y, z)]
    greeted = greet([to_core, to_x, to_y, *to_z, group[2]])

    wd_load = pltpu.make_async_copy(wd_any.at[0], wd, in_sem.at[2])

    def own_load(k):
        units = pl.ds(k, 1) if k == 0 else pl.ds(1, UNITS - 1)
        return pltpu.make_async_copy(u_any.at[units], u.at[units], in_sem.at[3 + k])

    def gu_load(k, t):
        first, units = CHUNKS[k]
        return pltpu.make_async_copy(gu_any.at[pl.ds(first, units), t], gu.at[t % 2, pl.ds(0, units)], in_sem.at[t % 2])

    def tile_loads(t):
        rows = pl.ds(WIDE * t, WIDE)
        return pltpu.make_async_copy(x_any.at[rows], a0.at[t], tile_sem.at[t, 0]), pltpu.make_async_copy(dh_any.at[t], dh.at[t], tile_sem.at[t, 1])

    for one in (own_load(0), own_load(1), wd_load, gu_load(0, 0), *tile_loads(0)):
        one.start()
    for t in range(1, 4):
        for one in tile_loads(t):
            one.start()
    squares[...] = jnp.zeros_like(squares)

    def c_copy(q):
        return remote(u.at[q, 1 - c], rc.at[q], s1.at[q, 0], r1.at[q, 0], to_core)

    def x_copy(q):
        return remote(sx.at[q], rx.at[q], s1.at[q, 1], r1.at[q, 1], to_x)

    def y_copy(q):
        return remote(sy.at[q], ry.at[q], s1.at[q, 2], r1.at[q, 2], to_y)

    def z_copy(q, k):
        return remote(sz.at[q, k], rz.at[q, k], s3.at[q, 0, k], r3.at[q, 0, k], to_z[k])

    def back_z_copy(q, k):
        return remote(g.at[q, 4 * y + z], g.at[q, 4 * y + z], s3.at[q, 1, k], r3.at[q, 1, k], to_z[k])

    def back_y_copy(q):
        half = g.at[q, pl.ds(4 * y, 4)]
        return remote(half, half, s1.at[q, 3], r1.at[q, 3], to_y)

    def upto_x(q, p):
        return u[q, c, x, p].astype(F32) + rc[q, x, p].astype(F32) + rx[q, p].astype(F32)

    def upto_y(q, k):
        return upto_x(q, 4 * y + k) + ry[q, k].astype(F32)

    def stage0(q):
        c_copy(q).start()

    def stage1(q):
        c_copy(q).wait_recv()
        sx[q] = (u[q, c, 1 - x].astype(F32) + rc[q, 1 - x].astype(F32)).astype(BF)
        x_copy(q).start()

    def stage2(q):
        x_copy(q).wait_recv()
        for k in range(4):
            sy[q, k] = upto_x(q, 4 * (1 - y) + k).astype(BF)
        y_copy(q).start()

    def stage3(q):
        y_copy(q).wait_recv()
        for k in range(3):
            sz[q, k] = upto_y(q, (z + k + 1) % 4).astype(BF)
        for k in range(3):
            z_copy(q, k).start()

    def stage4(q):
        for k in range(3):
            z_copy(q, k).wait_recv()
        total = upto_y(q, z)
        for k in range(3):
            total += rz[q, k].astype(F32)
        g[q, 4 * y + z] = total.astype(BF)
        for k in range(3):
            back_z_copy(q, k).start()

    def stage5(q):
        for k in range(3):
            back_z_copy(q, k).wait_recv()
        back_y_copy(q).start()

    def stage6(q):
        back_y_copy(q).wait_recv()
        wide = g[q].astype(F32).reshape(48, 8, LANE)
        squares[...] += jnp.sum(wide * wide, 0)

    stages = (stage0, stage1, stage2, stage3, stage4, stage5, stage6)

    def tick(m):
        for j in reversed(range(7)):
            q = m - max(2 * j - 1, 0)

            @pl.when((q >= 0) & (q < ALL))
            def _():
                stages[j](q)

    own_load(0).wait()
    greeted()
    tick(0)
    own_load(1).wait()
    wd_load.wait()
    for number, (first, units) in enumerate(CHUNKS):
        acc_d[...] = jnp.zeros_like(acc_d)
        acc_gu[...] = jnp.zeros_like(acc_gu)

        @pl.loop(0, 4)
        def _(t):
            @pl.when(t < 3)
            def _():
                gu_load(number, t + 1).start()

            if number < 3:

                @pl.when(t == 3)
                def _():
                    gu_load(number + 1, 0).start()

            gu_load(number, t).wait()
            if number == 0:
                for one in tile_loads(t):
                    one.wait()
                wide = a0[t].astype(F32)
                a0[t] = (wide * lax.rsqrt(jnp.mean(wide * wide, -1, keepdims=True) + 1e-6)).astype(BF)
            a, h = a0[t], dh[t]
            for n in range(units):
                d = nn(wd[first + n].reshape(LANE, D), h).astype(BF).astype(F32)
                one, dg, du = backward_unit(gu[t % 2, n, :LANE, :], gu[t % 2, n, LANE:, :], d)
                act[LANE * n : LANE * n + LANE, :] = one
                dgu[PAIR * n : PAIR * n + LANE, :] = dg
                dgu[PAIR * n + LANE : PAIR * n + PAIR, :] = du
            acc_d[: LANE * units, :] += nt(act[: LANE * units, :], h)
            acc_gu[: PAIR * units, :] += nn(dgu[: PAIR * units, :], a)

            tick(5 * number + t + 1)

        @pl.loop(0, units)
        def _(n):
            pack(UNITS + first + n, acc_gu, acc_d, n, u)

        tick(5 * number + 5)

    @pl.loop(21, ALL + 11)
    def _(m):
        tick(m)

    mine = sums.at[2 * x + c]
    norm = [remote(mine, mine, norm_send.at[k], norm_recv.at[k], group[k]) for k in range(3)]
    sums[2 * x + c] = squares[...]
    for one in norm:
        one.start()
    g_out[...] = g[...]

    @pl.loop(0, ALL)
    def _(q):
        for one in (c_copy(q), x_copy(q), y_copy(q), back_y_copy(q)):
            one.wait_send()
        for k in range(3):
            z_copy(q, k).wait_send()
            back_z_copy(q, k).wait_send()

    for one in norm:
        one.wait()
    total_out[...] = sums[0] + sums[1] + sums[2] + sums[3]


def third_kernel(g_ref, total_ref, *refs):
    weights, ms, vs = refs[0:3], refs[3:6], refs[6:9]
    outs, buffers = refs[9:18], refs[18:27]
    turned, plain, sem = refs[27:30]
    factor = jnp.minimum(1.0, 0.5 * lax.rsqrt(jnp.sum(total_ref[...]) / COUNT + 1e-30))

    def copies(l, i):
        return [pltpu.make_async_copy(buffers[k].at[l], outs[k].at[l], sem.at[l, k]) for k in (i, 3 + i, 6 + i)]

    def take(l, i, g):
        g = g * factor
        m = 0.9 * ms[i][l] + 0.1 * g
        v = 0.95 * vs[i][l] + 0.05 * g * g
        w = weights[i][l].astype(F32)
        buffers[3 + i][l] = m
        buffers[6 + i][l] = v
        buffers[i][l] = (w - 0.02 * (m * lax.rsqrt(v + 1e-8) + 0.1 * w)).astype(BF)
        for one in copies(l, i):
            one.start()

    for l in range(2):
        for n in range(UNITS):
            for p in range(8):
                row = SEG * n + 16 * (p // 4)
                plain[row : row + 16, LANE * (p % 4) : LANE * (p % 4) + LANE] = g_ref[1 - l, n, p, 32:48, :].astype(F32)
        take(l, 2, plain[...])
        for i in range(2):
            for n in range(UNITS):
                for s in range(4):
                    turned[352 * s + SEG * n : 352 * s + SEG * n + SEG, :] = g_ref[1 - l, n, 4 * i + s, 0:32, :].astype(F32)
            take(l, i, turned[...].T)
    for l in range(2):
        for i in range(3):
            for one in copies(l, i):
                one.wait()


def step(x, dy, w_gate, w_up, w_down, *moments):
    tokens = x.shape[1]
    tiles = tokens // TT
    any_ = pl.BlockSpec(memory_space=pl.ANY)

    def once(shape):
        return pl.BlockSpec(shape, lambda i: (0,) * len(shape), pipeline_mode=pl.Buffered(1))

    unit = (UNITS, 2, 2, 8, 48, LANE)
    dma = pltpu.SemaphoreType.DMA
    u1, dh, gu0, wd0 = pl.pallas_call(
        first_kernel,
        grid=(2 + tiles,),
        in_specs=[
            pl.BlockSpec((tiles // 2, TT, D), lambda i: (jnp.minimum(i, 1), 0, 0)),
            pl.BlockSpec((TT, D), lambda i: (jnp.maximum(i - 2, 0), 0)),
            once(w_gate.shape), once(w_up.shape), once(w_down.shape),
        ],
        out_specs=[once(unit), pl.BlockSpec((1, D, TT), lambda i: (jnp.maximum(i - 2, 0) // 2, 0, jnp.maximum(i - 2, 0) % 2)), any_, any_],
        out_shape=[
            jax.ShapeDtypeStruct(unit, BF),
            jax.ShapeDtypeStruct((tiles // 2, D, WIDE), BF),
            jax.ShapeDtypeStruct((UNITS, tiles // 2, PAIR, WIDE), F32),
            jax.ShapeDtypeStruct((2, UNITS, 4, SEG, D), BF),
        ],
        scratch_shapes=[
            pltpu.VMEM((2, UNITS, 2, LANE, D), BF),
            pltpu.VMEM((2, UNITS, 4, SEG, D), BF),
            pltpu.VMEM((tiles, D, TT), BF),
            pltpu.VMEM((tiles // 2, FF, TT), BF),
            pltpu.VMEM((tiles // 2, TT, D), BF),
            pltpu.VMEM((2, UNITS, PAIR, TT), F32),
            pltpu.VMEM((2 * FF, TT), BF),
            pltpu.VMEM((D, FF), BF),
            pltpu.VMEM((2 * FF, D), F32),
            pltpu.VMEM((FF, D), F32),
            dma((2, 2)), dma((2, 2)), dma((2, 5, 4)), dma((2, 5, 4)), dma((4, 2)), dma((1,)),
        ],
        compiler_params=pltpu.CompilerParams(vmem_limit_bytes=VMEM_LIMIT, collective_id=0, has_side_effects=True),
        name="gather_forward_and_last_layer",
    )(x.reshape(tiles, TT, D), dy[0], w_gate, w_up, w_down)

    most = max(units for _, units in CHUNKS)
    g, total = pl.pallas_call(
        second_kernel,
        in_specs=[pl.BlockSpec(memory_space=pltpu.HBM)] * 5,
        out_specs=[pl.BlockSpec(memory_space=pltpu.VMEM)] * 2,
        out_shape=[jax.ShapeDtypeStruct((ALL, 8, 48, LANE), BF), jax.ShapeDtypeStruct((8, LANE), F32)],
        scratch_shapes=[
            pltpu.VMEM((tiles // 2, WIDE, D), BF),
            pltpu.VMEM((tiles // 2, D, WIDE), BF),
            pltpu.VMEM((2, most, PAIR, WIDE), F32),
            pltpu.VMEM((UNITS, 4, SEG, D), BF),
            pltpu.VMEM((ALL, 2, 2, 8, 48, LANE), BF),
            pltpu.VMEM((LANE * most, WIDE), BF),
            pltpu.VMEM((PAIR * most, WIDE), BF),
            pltpu.VMEM((PAIR * most, D), F32),
            pltpu.VMEM((LANE * most, D), F32),
            pltpu.VMEM((ALL, 2, 8, 48, LANE), BF),
            pltpu.VMEM((ALL, 8, 48, LANE), BF),
            pltpu.VMEM((ALL, 8, 48, LANE), BF),
            pltpu.VMEM((ALL, 4, 48, LANE), BF),
            pltpu.VMEM((ALL, 4, 48, LANE), BF),
            pltpu.VMEM((ALL, 3, 48, LANE), BF),
            pltpu.VMEM((ALL, 3, 48, LANE), BF),
            pltpu.VMEM((ALL, 8, 48, LANE), BF),
            pltpu.VMEM((4, 8, LANE), F32),
            pltpu.VMEM((8, LANE), F32),
            dma((ALL, 4)), dma((ALL, 4)), dma((ALL, 2, 3)), dma((ALL, 2, 3)),
            dma((3,)), dma((3,)), dma((5,)), dma((tiles, 2)),
        ],
        compiler_params=pltpu.CompilerParams(vmem_limit_bytes=50 * MIB, collective_id=1, has_side_effects=True),
        name="first_layer_and_sums",
    )(x[0], dh, gu0, wd0, u1)

    arrays = (w_gate, w_up, w_down, *moments)

    vmem = pl.BlockSpec(memory_space=pltpu.VMEM)
    return pl.pallas_call(
        third_kernel,
        in_specs=[vmem] * (2 + len(arrays)),
        out_specs=[any_] * len(arrays),
        out_shape=[jax.ShapeDtypeStruct(a.shape, a.dtype) for a in arrays],
        scratch_shapes=[pltpu.VMEM(a.shape, a.dtype) for a in arrays]
        + [pltpu.VMEM((FF, LANE), F32), pltpu.VMEM((FF // 4, D), F32), dma((2, 9))],
        compiler_params=pltpu.CompilerParams(vmem_limit_bytes=28 * MIB),
        name="clip_and_adamw",
    )(g.reshape(2, UNITS, 8, 48, LANE), total, *arrays)


def solution(mesh):
    states, cut = P(("rep", "r", "s"), None, None), P(None, "s", None)
    return jax.shard_map(
        lambda *arrays: tuple(step(*arrays)),
        mesh=mesh,
        in_specs=(states, states) + (cut,) * 9,
        out_specs=(P("rep", "s", None),) * 9,
        check_vma=False,
    )
```

```python
import functools

import jax
import jax.numpy as jnp
from jax import lax
from jax.experimental import pallas as pl
from jax.experimental.pallas import tpu as pltpu
from jax.sharding import PartitionSpec as P

F32, BF = jnp.float32, jnp.bfloat16
D, FF, TT, WIDE = 512, 1408, 512, 1024
UNITS, SEG = 11, 32
ALL = 2 * UNITS
CHUNKS = ((0, 3), (3, 3), (6, 3), (9, 2))
COUNT = 2 * 3 * D * FF
MIB = 2**20
VMEM_LIMIT = 62 * MIB
LANE, PAIR = 128, 256


def nn(a, b):
    return lax.dot_general(a, b, (((1,), (0,)), ((), ())), preferred_element_type=F32)


def nt(a, b):
    return lax.dot_general(a, b, (((1,), (1,)), ((), ())), preferred_element_type=F32)


def sigmoid(g):
    return 0.5 * jnp.tanh(0.5 * g) + 0.5


def backward_unit(g, u, d):
    s = sigmoid(g)
    silu = g * s
    return (silu * u).astype(BF), (d * u * (s + silu * (1.0 - s))).astype(BF), (d * silu).astype(BF)


def place():
    r, s = lax.axis_index("r"), lax.axis_index("s")
    return s // 2, s % 2, r // 4, r % 4


def device(x, core, y, z):
    return (0, y * 4 + z, x * 2 + core)


def remote(src, dst, send, recv, where):
    return pltpu.make_async_remote_copy(
        src_ref=src, dst_ref=dst, send_sem=send, recv_sem=recv, device_id=where, device_id_type=pl.DeviceIdType.MESH
    )


def greet(peers):
    barrier = pltpu.get_barrier_semaphore()
    for peer in peers:
        pl.semaphore_signal(barrier, inc=1, device_id=peer, device_id_type=pl.DeviceIdType.MESH)
    return lambda: pl.semaphore_wait(barrier, len(peers))


def pack(n, acc_gu, acc_d, row, out):
    for core in range(2):
        for x in range(2):
            s = 2 * x + core
            for p in range(8):
                y, z = p // 4, p % 4
                gu = pl.ds(pl.multiple_of(PAIR * row + 32 * p, 32), 32)
                d = pl.ds(pl.multiple_of(LANE * row + SEG * s + 16 * y, 16), 16)
                out[n, core, x, p, 0:32, :] = acc_gu[gu, LANE * s : LANE * s + LANE].astype(BF)
                out[n, core, x, p, 32:48, :] = acc_d[d, LANE * z : LANE * z + LANE].astype(BF)


def first_kernel(
    x_ref, dy_ref, gate_ref, up_ref, down_ref, u_ref, dh_ref, gu_out, wd_out,
    wgu, wd, h1s, acts, a_first, stage, dgu, wdt, acc_gu, acc_d, own_send, own_recv, send, recv, gu_sem, out_sem,
):
    i = pl.program_id(0)
    x, c, y, z = place()
    me, far = 2 * x + c, 2 * (1 - x) + c
    to_core, to_x, to_y = device(x, 1 - c, y, z), device(1 - x, c, y, z), device(x, c, 1 - y, z)

    def lanes(s):
        return pl.ds(pl.multiple_of(LANE * s, LANE), LANE)

    def piece(l, p, s, half):
        if p == 4:
            return wd.at[l, :, s, pl.ds(pl.multiple_of(16 * half, 16), 16), :]
        first, units = CHUNKS[p]
        return wgu.at[l, pl.ds(first, units), half, :, lanes(s)]

    def copy(l, p, stage):
        half = 1 - y if stage == 3 else y
        ref = piece(l, p, me if stage == 0 else far, half)
        return remote(ref, ref, send.at[l, p, stage], recv.at[l, p, stage], (to_x, to_y, to_core, to_core)[stage])

    def own(l, k):
        ref = wd.at[l, :, me] if k else wgu.at[l, :, :, :, lanes(me)]
        return remote(ref, ref, own_send.at[l, k], own_recv.at[l, k], to_core)

    wd_copy = pltpu.make_async_copy(wd, wd_out, out_sem.at[0])

    def gu_copy(p, t):
        first, units = CHUNKS[p]
        rows = pl.ds(first, units)
        there = gu_out.at[rows, t // 2, :, pl.ds(pl.multiple_of(TT * (t % 2), TT), TT)]
        return pltpu.make_async_copy(stage.at[t % 2, rows], there, gu_sem.at[p, t % 2])

    def from_x(l, p):
        copy(l, p, 0).wait_recv()
        copy(l, p, 1).start()
        copy(l, p, 2).start()

    def from_y(l, p):
        copy(l, p, 1).wait_recv()
        copy(l, p, 3).start()

    def arrived(l, p):
        for stage in (2, 3):
            copy(l, p, stage).wait_recv()

    def place_own(l):
        for g, ref in enumerate((gate_ref, up_ref)):
            turned = ref[l].T
            for n in range(UNITS):
                for s in range(4):
                    wgu[l, n, g, SEG * s : SEG * s + SEG, lanes(me)] = turned[
                        352 * s + SEG * n : 352 * s + SEG * n + SEG, :
                    ]
        wd[l, :, me] = down_ref[l].reshape(UNITS, SEG, D)

    def up_and_gate(first, units, a, out, slot):
        for n in range(first, first + units):
            gu = nt(wgu[0, n].reshape(PAIR, D), a)
            stage[slot, n] = gu
            out[LANE * n : LANE * n + LANE, :] = (gu[:LANE] * sigmoid(gu[:LANE]) * gu[LANE:]).astype(BF)

    def down(x, act, t):
        h1s[t] = (x.T.astype(F32) + nn(wdt[...], act[...]).astype(BF).astype(F32)).astype(BF)

    @pl.when(i == 0)
    def _():
        greeted = greet((to_core, to_x, to_y))
        place_own(0)
        greeted()
        for l in range(2):
            if l:
                place_own(1)
            for k in range(2):
                own(l, k).start()
            for p in range(5):
                copy(l, p, 0).start()
        acc_gu[...] = jnp.zeros_like(acc_gu)
        acc_d[...] = jnp.zeros_like(acc_d)
        own(0, 0).wait_recv()
        from_x(0, 0)
        from_x(0, 1)
        for p in range(4):
            if p < 3:
                from_x(0, p + 2)
            else:
                from_x(1, 0)
            from_y(0, p)
            arrived(0, p)
            first, units = CHUNKS[p]

            @pl.loop(0, 4)
            def _(t):
                if p == 0:
                    wide = x_ref[t].astype(F32)
                    a_first[t] = (wide * lax.rsqrt(jnp.mean(wide * wide, -1, keepdims=True) + 1e-6)).astype(BF)

                @pl.when(t >= 2)
                def _():
                    gu_copy(p, t - 2).wait()

                up_and_gate(first, units, a_first[t], acts.at[t], t % 2)
                gu_copy(p, t).start()

        from_x(1, 1)
        from_y(0, 4)
        own(0, 1).wait_recv()
        arrived(0, 4)
        wdt[...] = wd[0].reshape(FF, D).T

        @pl.loop(0, 4)
        def _(t):
            for p in range(2):

                @pl.when(t == p)
                def _():
                    from_x(1, p + 2)
                    from_y(1, p)

            down(x_ref[t], acts.at[t], t)

    @pl.when(i == 1)
    def _():
        @pl.loop(0, 4)
        def _(t):
            @pl.when(t == 0)
            def _():
                from_x(1, 4)

            for p in range(2, 5):

                @pl.when(t == p - 1)
                def _():
                    from_y(1, p)

            x = x_ref[t]
            wide = x.astype(F32)
            a = (wide * lax.rsqrt(jnp.mean(wide * wide, -1, keepdims=True) + 1e-6)).astype(BF)
            for p in range(4):
                gu_copy(p, t + 2).wait()
            up_and_gate(0, UNITS, a, acts.at[0], t % 2)
            for p in range(4):
                gu_copy(p, t + 4).start()
            down(x, acts.at[0], 4 + t)

        for k in range(2):
            own(1, k).wait_recv()
        for p in range(5):
            arrived(1, p)
        wd_copy.start()

    @pl.when(i >= 2)
    def _():
        act = acts.at[0]
        wide = h1s[i - 2].astype(F32)
        scale = lax.rsqrt(jnp.mean(wide * wide, 0, keepdims=True) + 1e-6)
        a = (wide * scale).astype(BF)
        dy = dy_ref[...]
        dyt = dy.T
        for n in range(UNITS):
            gu = nn(wgu[1, n].reshape(PAIR, D), a)
            d = nn(wd[1, n].reshape(LANE, D), dyt).astype(BF).astype(F32)
            one, dg, du = backward_unit(gu[:LANE], gu[LANE:], d)
            act[LANE * n : LANE * n + LANE, :] = one
            dgu[PAIR * n : PAIR * n + LANE, :] = dg
            dgu[PAIR * n + LANE : PAIR * n + PAIR, :] = du
        acc_d[...] += nn(act[...], dy)
        acc_gu[...] += nt(dgu[...], a)
        da = lax.dot_general(wgu[1].reshape(2 * FF, D), dgu[...], (((0,), (0,)), ((), ())), preferred_element_type=F32).astype(BF).astype(F32)
        back = scale * da - wide * (scale * scale * scale * jnp.mean(wide * da, 0, keepdims=True))
        dh_ref[0] = (dyt.astype(F32) + back.astype(BF).astype(F32)).astype(BF)

    @pl.when(i == 9)
    def _():
        @pl.loop(0, UNITS)
        def _(n):
            pack(n, acc_gu, acc_d, n, u_ref)

        wd_copy.wait()
        for p in range(4):
            for t in (6, 7):
                gu_copy(p, t).wait()
        for l in range(2):
            for k in range(2):
                own(l, k).wait_send()
            for p in range(5):
                for stage in range(4):
                    copy(l, p, stage).wait_send()


def second_kernel(
    x_any, dh_any, gu_any, wd_any, u_any, g_out, total_out,
    a0, dh, gu, wd, u, act, dgu, acc_gu, acc_d,
    rc, sx, rx, sy, ry, sz, rz, g, sums, squares,
    s1, r1, s3, r3, norm_send, norm_recv, in_sem, tile_sem,
):
    x, c, y, z = place()
    to_core, to_x, to_y = device(x, 1 - c, y, z), device(1 - x, c, y, z), device(x, c, 1 - y, z)
    to_z = [device(x, c, y, (z + k) % 4) for k in (1, 2, 3)]
    group = [to_core, to_x, device(1 - x, 1 - c, y, z)]
    greeted = greet([to_core, to_x, to_y, *to_z, group[2]])

    wd_load = pltpu.make_async_copy(wd_any.at[0], wd, in_sem.at[2])

    def own_load(k):
        units = pl.ds(k, 1) if k == 0 else pl.ds(1, UNITS - 1)
        return pltpu.make_async_copy(u_any.at[units], u.at[units], in_sem.at[3 + k])

    def gu_load(k, t):
        first, units = CHUNKS[k]
        return pltpu.make_async_copy(gu_any.at[pl.ds(first, units), t], gu.at[t % 2, pl.ds(0, units)], in_sem.at[t % 2])

    def tile_loads(t):
        rows = pl.ds(WIDE * t, WIDE)
        return pltpu.make_async_copy(x_any.at[rows], a0.at[t], tile_sem.at[t, 0]), pltpu.make_async_copy(dh_any.at[t], dh.at[t], tile_sem.at[t, 1])

    for one in (own_load(0), own_load(1), wd_load, gu_load(0, 0), *tile_loads(0)):
        one.start()
    for t in range(1, 4):
        for one in tile_loads(t):
            one.start()
    squares[...] = jnp.zeros_like(squares)

    def c_copy(q):
        return remote(u.at[q, 1 - c], rc.at[q], s1.at[q, 0], r1.at[q, 0], to_core)

    def x_copy(q):
        return remote(sx.at[q], rx.at[q], s1.at[q, 1], r1.at[q, 1], to_x)

    def y_copy(q):
        return remote(sy.at[q], ry.at[q], s1.at[q, 2], r1.at[q, 2], to_y)

    def z_copy(q, k):
        return remote(sz.at[q, k], rz.at[q, k], s3.at[q, 0, k], r3.at[q, 0, k], to_z[k])

    def back_z_copy(q, k):
        return remote(g.at[q, 4 * y + z], g.at[q, 4 * y + z], s3.at[q, 1, k], r3.at[q, 1, k], to_z[k])

    def back_y_copy(q):
        half = g.at[q, pl.ds(4 * y, 4)]
        return remote(half, half, s1.at[q, 3], r1.at[q, 3], to_y)

    def upto_x(q, p):
        return u[q, c, x, p].astype(F32) + rc[q, x, p].astype(F32) + rx[q, p].astype(F32)

    def upto_y(q, k):
        return upto_x(q, 4 * y + k) + ry[q, k].astype(F32)

    def stage0(q):
        c_copy(q).start()

    def stage1(q):
        c_copy(q).wait_recv()
        sx[q] = (u[q, c, 1 - x].astype(F32) + rc[q, 1 - x].astype(F32)).astype(BF)
        x_copy(q).start()

    def stage2(q):
        x_copy(q).wait_recv()
        for k in range(4):
            sy[q, k] = upto_x(q, 4 * (1 - y) + k).astype(BF)
        y_copy(q).start()

    def stage3(q):
        y_copy(q).wait_recv()
        for k in range(3):
            sz[q, k] = upto_y(q, (z + k + 1) % 4).astype(BF)
        for k in range(3):
            z_copy(q, k).start()

    def stage4(q):
        for k in range(3):
            z_copy(q, k).wait_recv()
        total = upto_y(q, z)
        for k in range(3):
            total += rz[q, k].astype(F32)
        g[q, 4 * y + z] = total.astype(BF)
        for k in range(3):
            back_z_copy(q, k).start()

    def stage5(q):
        for k in range(3):
            back_z_copy(q, k).wait_recv()
        back_y_copy(q).start()

    def stage6(q):
        back_y_copy(q).wait_recv()
        wide = g[q].astype(F32).reshape(48, 8, LANE)
        squares[...] += jnp.sum(wide * wide, 0)

    stages = (stage0, stage1, stage2, stage3, stage4, stage5, stage6)

    def tick(m):
        for j in reversed(range(7)):
            q = m - max(2 * j - 1, 0)

            @pl.when((q >= 0) & (q < ALL))
            def _():
                stages[j](q)

    own_load(0).wait()
    greeted()
    tick(0)
    own_load(1).wait()
    wd_load.wait()
    for number, (first, units) in enumerate(CHUNKS):
        acc_d[...] = jnp.zeros_like(acc_d)
        acc_gu[...] = jnp.zeros_like(acc_gu)

        @pl.loop(0, 4)
        def _(t):
            @pl.when(t < 3)
            def _():
                gu_load(number, t + 1).start()

            if number < 3:

                @pl.when(t == 3)
                def _():
                    gu_load(number + 1, 0).start()

            gu_load(number, t).wait()
            if number == 0:
                for one in tile_loads(t):
                    one.wait()
                wide = a0[t].astype(F32)
                a0[t] = (wide * lax.rsqrt(jnp.mean(wide * wide, -1, keepdims=True) + 1e-6)).astype(BF)
            a, h = a0[t], dh[t]
            for n in range(units):
                d = nn(wd[first + n].reshape(LANE, D), h).astype(BF).astype(F32)
                one, dg, du = backward_unit(gu[t % 2, n, :LANE, :], gu[t % 2, n, LANE:, :], d)
                act[LANE * n : LANE * n + LANE, :] = one
                dgu[PAIR * n : PAIR * n + LANE, :] = dg
                dgu[PAIR * n + LANE : PAIR * n + PAIR, :] = du
            acc_d[: LANE * units, :] += nt(act[: LANE * units, :], h)
            acc_gu[: PAIR * units, :] += nn(dgu[: PAIR * units, :], a)

            tick(5 * number + t + 1)

        @pl.loop(0, units)
        def _(n):
            pack(UNITS + first + n, acc_gu, acc_d, n, u)

        tick(5 * number + 5)

    @pl.loop(21, ALL + 11)
    def _(m):
        tick(m)

    mine = sums.at[2 * x + c]
    norm = [remote(mine, mine, norm_send.at[k], norm_recv.at[k], group[k]) for k in range(3)]
    sums[2 * x + c] = squares[...]
    for one in norm:
        one.start()
    g_out[...] = g[...]

    @pl.loop(0, ALL)
    def _(q):
        for one in (c_copy(q), x_copy(q), y_copy(q), back_y_copy(q)):
            one.wait_send()
        for k in range(3):
            z_copy(q, k).wait_send()
            back_z_copy(q, k).wait_send()

    for one in norm:
        one.wait()
    total_out[...] = sums[0] + sums[1] + sums[2] + sums[3]


def third_kernel(g_ref, total_ref, *refs):
    weights, ms, vs = refs[0:3], refs[3:6], refs[6:9]
    outs, buffers = refs[9:18], refs[18:27]
    turned, plain, sem = refs[27:30]
    factor = jnp.minimum(1.0, 0.5 * lax.rsqrt(jnp.sum(total_ref[...]) / COUNT + 1e-30))

    def copies(l, i):
        return [pltpu.make_async_copy(buffers[k].at[l], outs[k].at[l], sem.at[l, k]) for k in (i, 3 + i, 6 + i)]

    def take(l, i, g):
        g = g * factor
        m = 0.9 * ms[i][l] + 0.1 * g
        v = 0.95 * vs[i][l] + 0.05 * g * g
        w = weights[i][l].astype(F32)
        buffers[3 + i][l] = m
        buffers[6 + i][l] = v
        buffers[i][l] = (w - 0.02 * (m * lax.rsqrt(v + 1e-8) + 0.1 * w)).astype(BF)
        for one in copies(l, i):
            one.start()

    for l in range(2):
        for n in range(UNITS):
            for p in range(8):
                row = SEG * n + 16 * (p // 4)
                plain[row : row + 16, LANE * (p % 4) : LANE * (p % 4) + LANE] = g_ref[1 - l, n, p, 32:48, :].astype(F32)
        take(l, 2, plain[...])
        for i in range(2):
            for n in range(UNITS):
                for s in range(4):
                    turned[352 * s + SEG * n : 352 * s + SEG * n + SEG, :] = g_ref[1 - l, n, 4 * i + s, 0:32, :].astype(F32)
            take(l, i, turned[...].T)
    for l in range(2):
        for i in range(3):
            for one in copies(l, i):
                one.wait()


def step(x, dy, w_gate, w_up, w_down, *moments):
    tokens = x.shape[1]
    tiles = tokens // TT
    any_ = pl.BlockSpec(memory_space=pl.ANY)

    def once(shape):
        return pl.BlockSpec(shape, lambda i: (0,) * len(shape), pipeline_mode=pl.Buffered(1))

    unit = (UNITS, 2, 2, 8, 48, LANE)
    dma = pltpu.SemaphoreType.DMA
    u1, dh, gu0, wd0 = pl.pallas_call(
        first_kernel,
        grid=(2 + tiles,),
        in_specs=[
            pl.BlockSpec((tiles // 2, TT, D), lambda i: (jnp.minimum(i, 1), 0, 0)),
            pl.BlockSpec((TT, D), lambda i: (jnp.maximum(i - 2, 0), 0)),
            once(w_gate.shape), once(w_up.shape), once(w_down.shape),
        ],
        out_specs=[once(unit), pl.BlockSpec((1, D, TT), lambda i: (jnp.maximum(i - 2, 0) // 2, 0, jnp.maximum(i - 2, 0) % 2)), any_, any_],
        out_shape=[
            jax.ShapeDtypeStruct(unit, BF),
            jax.ShapeDtypeStruct((tiles // 2, D, WIDE), BF),
            jax.ShapeDtypeStruct((UNITS, tiles // 2, PAIR, WIDE), F32),
            jax.ShapeDtypeStruct((2, UNITS, 4, SEG, D), BF),
        ],
        scratch_shapes=[
            pltpu.VMEM((2, UNITS, 2, LANE, D), BF),
            pltpu.VMEM((2, UNITS, 4, SEG, D), BF),
            pltpu.VMEM((tiles, D, TT), BF),
            pltpu.VMEM((tiles // 2, FF, TT), BF),
            pltpu.VMEM((tiles // 2, TT, D), BF),
            pltpu.VMEM((2, UNITS, PAIR, TT), F32),
            pltpu.VMEM((2 * FF, TT), BF),
            pltpu.VMEM((D, FF), BF),
            pltpu.VMEM((2 * FF, D), F32),
            pltpu.VMEM((FF, D), F32),
            dma((2, 2)), dma((2, 2)), dma((2, 5, 4)), dma((2, 5, 4)), dma((4, 2)), dma((1,)),
        ],
        compiler_params=pltpu.CompilerParams(vmem_limit_bytes=VMEM_LIMIT, collective_id=0, has_side_effects=True),
        name="gather_forward_and_last_layer",
    )(x.reshape(tiles, TT, D), dy[0], w_gate, w_up, w_down)

    most = max(units for _, units in CHUNKS)
    g, total = pl.pallas_call(
        second_kernel,
        in_specs=[pl.BlockSpec(memory_space=pltpu.HBM)] * 5,
        out_specs=[pl.BlockSpec(memory_space=pltpu.VMEM)] * 2,
        out_shape=[jax.ShapeDtypeStruct((ALL, 8, 48, LANE), BF), jax.ShapeDtypeStruct((8, LANE), F32)],
        scratch_shapes=[
            pltpu.VMEM((tiles // 2, WIDE, D), BF),
            pltpu.VMEM((tiles // 2, D, WIDE), BF),
            pltpu.VMEM((2, most, PAIR, WIDE), F32),
            pltpu.VMEM((UNITS, 4, SEG, D), BF),
            pltpu.VMEM((ALL, 2, 2, 8, 48, LANE), BF),
            pltpu.VMEM((LANE * most, WIDE), BF),
            pltpu.VMEM((PAIR * most, WIDE), BF),
            pltpu.VMEM((PAIR * most, D), F32),
            pltpu.VMEM((LANE * most, D), F32),
            pltpu.VMEM((ALL, 2, 8, 48, LANE), BF),
            pltpu.VMEM((ALL, 8, 48, LANE), BF),
            pltpu.VMEM((ALL, 8, 48, LANE), BF),
            pltpu.VMEM((ALL, 4, 48, LANE), BF),
            pltpu.VMEM((ALL, 4, 48, LANE), BF),
            pltpu.VMEM((ALL, 3, 48, LANE), BF),
            pltpu.VMEM((ALL, 3, 48, LANE), BF),
            pltpu.VMEM((ALL, 8, 48, LANE), BF),
            pltpu.VMEM((4, 8, LANE), F32),
            pltpu.VMEM((8, LANE), F32),
            dma((ALL, 4)), dma((ALL, 4)), dma((ALL, 2, 3)), dma((ALL, 2, 3)),
            dma((3,)), dma((3,)), dma((5,)), dma((tiles, 2)),
        ],
        compiler_params=pltpu.CompilerParams(vmem_limit_bytes=50 * MIB, collective_id=1, has_side_effects=True),
        name="first_layer_and_sums",
    )(x[0], dh, gu0, wd0, u1)

    arrays = (w_gate, w_up, w_down, *moments)

    vmem = pl.BlockSpec(memory_space=pltpu.VMEM)
    return pl.pallas_call(
        third_kernel,
        in_specs=[vmem] * (2 + len(arrays)),
        out_specs=[any_] * len(arrays),
        out_shape=[jax.ShapeDtypeStruct(a.shape, a.dtype) for a in arrays],
        scratch_shapes=[pltpu.VMEM(a.shape, a.dtype) for a in arrays]
        + [pltpu.VMEM((FF, LANE), F32), pltpu.VMEM((FF // 4, D), F32), dma((2, 9))],
        compiler_params=pltpu.CompilerParams(vmem_limit_bytes=28 * MIB),
        name="clip_and_adamw",
    )(g.reshape(2, UNITS, 8, 48, LANE), total, *arrays)


def solution(mesh):
    states, cut = P(("rep", "r", "s"), None, None), P(None, "s", None)
    return jax.shard_map(
        lambda *arrays: tuple(step(*arrays)),
        mesh=mesh,
        in_specs=(states, states) + (cut,) * 9,
        out_specs=(P("rep", "s", None),) * 9,
        check_vma=False,
    )
```

```python
import functools

import jax
import jax.numpy as jnp
from jax import lax
from jax.experimental import pallas as pl
from jax.experimental.pallas import tpu as pltpu
from jax.sharding import PartitionSpec as P

F32, BF = jnp.float32, jnp.bfloat16
D, FF, TT, WIDE = 512, 1408, 512, 1024
UNITS, SEG = 11, 32
ALL = 2 * UNITS
CHUNKS = ((0, 3), (3, 3), (6, 3), (9, 2))
COUNT = 2 * 3 * D * FF
MIB = 2**20
VMEM_LIMIT = 62 * MIB
LANE, PAIR = 128, 256


def nn(a, b):
    return lax.dot_general(a, b, (((1,), (0,)), ((), ())), preferred_element_type=F32)


def nt(a, b):
    return lax.dot_general(a, b, (((1,), (1,)), ((), ())), preferred_element_type=F32)


def sigmoid(g):
    return 0.5 * jnp.tanh(0.5 * g) + 0.5


def backward_unit(g, u, d):
    s = sigmoid(g)
    silu = g * s
    return (silu * u).astype(BF), (d * u * (s + silu * (1.0 - s))).astype(BF), (d * silu).astype(BF)


def place():
    r, s = lax.axis_index("r"), lax.axis_index("s")
    return s // 2, s % 2, r // 4, r % 4


def device(x, core, y, z):
    return (0, y * 4 + z, x * 2 + core)


def remote(src, dst, send, recv, where):
    return pltpu.make_async_remote_copy(
        src_ref=src, dst_ref=dst, send_sem=send, recv_sem=recv, device_id=where, device_id_type=pl.DeviceIdType.MESH
    )


def greet(peers):
    barrier = pltpu.get_barrier_semaphore()
    for peer in peers:
        pl.semaphore_signal(barrier, inc=1, device_id=peer, device_id_type=pl.DeviceIdType.MESH)
    return lambda: pl.semaphore_wait(barrier, len(peers))


def pack(n, acc_gu, acc_d, row, out):
    for core in range(2):
        for x in range(2):
            s = 2 * x + core
            for p in range(8):
                y, z = p // 4, p % 4
                gu = pl.ds(pl.multiple_of(PAIR * row + 32 * p, 32), 32)
                d = pl.ds(pl.multiple_of(LANE * row + SEG * s + 16 * y, 16), 16)
                out[n, core, x, p, 0:32, :] = acc_gu[gu, LANE * s : LANE * s + LANE].astype(BF)
                out[n, core, x, p, 32:48, :] = acc_d[d, LANE * z : LANE * z + LANE].astype(BF)


def first_kernel(
    x_ref, dy_ref, gate_ref, up_ref, down_ref, u_out, dh_ref, gu_out, wd_out,
    u, wgu, wd, h1s, acts, a_first, stage, dgu, wdt, acc_gu, acc_d, own_send, own_recv, send, recv, gu_sem, u_sem, out_sem,
):
    i = pl.program_id(0)
    x, c, y, z = place()
    me, far = 2 * x + c, 2 * (1 - x) + c
    to_core, to_x, to_y = device(x, 1 - c, y, z), device(1 - x, c, y, z), device(x, c, 1 - y, z)

    def lanes(s):
        return pl.ds(pl.multiple_of(LANE * s, LANE), LANE)

    def piece(l, p, s, half):
        if p == 4:
            return wd.at[l, :, s, pl.ds(pl.multiple_of(16 * half, 16), 16), :]
        first, units = CHUNKS[p]
        return wgu.at[l, pl.ds(first, units), half, :, lanes(s)]

    def copy(l, p, stage):
        half = 1 - y if stage == 3 else y
        ref = piece(l, p, me if stage == 0 else far, half)
        return remote(ref, ref, send.at[l, p, stage], recv.at[l, p, stage], (to_x, to_y, to_core, to_core)[stage])

    def own(l, k):
        ref = wd.at[l, :, me] if k else wgu.at[l, :, :, :, lanes(me)]
        return remote(ref, ref, own_send.at[l, k], own_recv.at[l, k], to_core)

    wd_copy = pltpu.make_async_copy(wd, wd_out, out_sem.at[0])

    def u_copy(n):
        return pltpu.make_async_copy(u.at[n], u_out.at[n], u_sem.at[n])

    def gu_copy(p, t):
        first, units = CHUNKS[p]
        rows = pl.ds(first, units)
        there = gu_out.at[rows, t // 2, :, pl.ds(pl.multiple_of(TT * (t % 2), TT), TT)]
        return pltpu.make_async_copy(stage.at[t % 2, rows], there, gu_sem.at[p, t % 2])

    def from_x(l, p):
        copy(l, p, 0).wait_recv()
        copy(l, p, 1).start()
        copy(l, p, 2).start()

    def from_y(l, p):
        copy(l, p, 1).wait_recv()
        copy(l, p, 3).start()

    def arrived(l, p):
        for stage in (2, 3):
            copy(l, p, stage).wait_recv()

    def place_own(l):
        for g, ref in enumerate((gate_ref, up_ref)):
            turned = ref[l].T
            for n in range(UNITS):
                for s in range(4):
                    wgu[l, n, g, SEG * s : SEG * s + SEG, lanes(me)] = turned[
                        352 * s + SEG * n : 352 * s + SEG * n + SEG, :
                    ]
        wd[l, :, me] = down_ref[l].reshape(UNITS, SEG, D)

    def up_and_gate(first, units, a, out, slot):
        for n in range(first, first + units):
            gu = nt(wgu[0, n].reshape(PAIR, D), a)
            stage[slot, n] = gu
            out[LANE * n : LANE * n + LANE, :] = (gu[:LANE] * sigmoid(gu[:LANE]) * gu[LANE:]).astype(BF)

    def down(x, act, t):
        h1s[t] = (x.T.astype(F32) + nn(wdt[...], act[...]).astype(BF).astype(F32)).astype(BF)

    @pl.when(i == 0)
    def _():
        greeted = greet((to_core, to_x, to_y))
        place_own(0)
        greeted()
        for l in range(2):
            if l:
                place_own(1)
            for k in range(2):
                own(l, k).start()
            for p in range(5):
                copy(l, p, 0).start()
        acc_gu[...] = jnp.zeros_like(acc_gu)
        acc_d[...] = jnp.zeros_like(acc_d)
        own(0, 0).wait_recv()
        from_x(0, 0)
        from_x(0, 1)
        for p in range(4):
            if p < 3:
                from_x(0, p + 2)
            else:
                from_x(1, 0)
            from_y(0, p)
            arrived(0, p)
            first, units = CHUNKS[p]

            @pl.loop(0, 4)
            def _(t):
                if p == 0:
                    wide = x_ref[t].astype(F32)
                    a_first[t] = (wide * lax.rsqrt(jnp.mean(wide * wide, -1, keepdims=True) + 1e-6)).astype(BF)

                @pl.when(t >= 2)
                def _():
                    gu_copy(p, t - 2).wait()

                up_and_gate(first, units, a_first[t], acts.at[t], t % 2)
                gu_copy(p, t).start()

        from_x(1, 1)
        from_y(0, 4)
        own(0, 1).wait_recv()
        arrived(0, 4)
        wdt[...] = wd[0].reshape(FF, D).T

        @pl.loop(0, 4)
        def _(t):
            for p in range(2):

                @pl.when(t == p)
                def _():
                    from_x(1, p + 2)
                    from_y(1, p)

            down(x_ref[t], acts.at[t], t)

    @pl.when(i == 1)
    def _():
        @pl.loop(0, 4)
        def _(t):
            @pl.when(t == 0)
            def _():
                from_x(1, 4)

            for p in range(2, 5):

                @pl.when(t == p - 1)
                def _():
                    from_y(1, p)

            x = x_ref[t]
            wide = x.astype(F32)
            a = (wide * lax.rsqrt(jnp.mean(wide * wide, -1, keepdims=True) + 1e-6)).astype(BF)
            for p in range(4):
                gu_copy(p, t + 2).wait()
            up_and_gate(0, UNITS, a, acts.at[0], t % 2)
            for p in range(4):
                gu_copy(p, t + 4).start()
            down(x, acts.at[0], 4 + t)

        for k in range(2):
            own(1, k).wait_recv()
        for p in range(5):
            arrived(1, p)
        wd_copy.start()

    @pl.when(i >= 2)
    def _():
        act = acts.at[0]
        wide = h1s[i - 2].astype(F32)
        scale = lax.rsqrt(jnp.mean(wide * wide, 0, keepdims=True) + 1e-6)
        a = (wide * scale).astype(BF)
        dy = dy_ref[...]
        dyt = dy.T
        for n in range(UNITS):
            gu = nn(wgu[1, n].reshape(PAIR, D), a)
            d = nn(wd[1, n].reshape(LANE, D), dyt).astype(BF).astype(F32)
            one, dg, du = backward_unit(gu[:LANE], gu[LANE:], d)
            act[LANE * n : LANE * n + LANE, :] = one
            dgu[PAIR * n : PAIR * n + LANE, :] = dg
            dgu[PAIR * n + LANE : PAIR * n + PAIR, :] = du
        acc_d[...] += nn(act[...], dy)
        acc_gu[...] += nt(dgu[...], a)
        da = lax.dot_general(wgu[1].reshape(2 * FF, D), dgu[...], (((0,), (0,)), ((), ())), preferred_element_type=F32).astype(BF).astype(F32)
        back = scale * da - wide * (scale * scale * scale * jnp.mean(wide * da, 0, keepdims=True))
        dh_ref[0] = (dyt.astype(F32) + back.astype(BF).astype(F32)).astype(BF)

    @pl.when(i == 9)
    def _():
        @pl.loop(0, UNITS)
        def _(n):
            pack(n, acc_gu, acc_d, n, u)
            u_copy(n).start()

        wd_copy.wait()
        for n in range(UNITS):
            u_copy(n).wait()
        for p in range(4):
            for t in (6, 7):
                gu_copy(p, t).wait()
        for l in range(2):
            for k in range(2):
                own(l, k).wait_send()
            for p in range(5):
                for stage in range(4):
                    copy(l, p, stage).wait_send()


def second_kernel(
    x_any, dh_any, gu_any, wd_any, u_any, g_out, total_out,
    a0, dh, gu, wd, u, act, dgu, acc_gu, acc_d,
    rc, sx, rx, sy, ry, sz, rz, g, sums, squares,
    s1, r1, s3, r3, norm_send, norm_recv, in_sem, tile_sem,
):
    x, c, y, z = place()
    to_core, to_x, to_y = device(x, 1 - c, y, z), device(1 - x, c, y, z), device(x, c, 1 - y, z)
    to_z = [device(x, c, y, (z + k) % 4) for k in (1, 2, 3)]
    group = [to_core, to_x, device(1 - x, 1 - c, y, z)]
    greeted = greet([to_core, to_x, to_y, *to_z, group[2]])

    wd_load = pltpu.make_async_copy(wd_any.at[0], wd, in_sem.at[2])

    def own_load(k):
        units = pl.ds(k, 1) if k == 0 else pl.ds(1, UNITS - 1)
        return pltpu.make_async_copy(u_any.at[units], u.at[units], in_sem.at[3 + k])

    def gu_load(k, t):
        first, units = CHUNKS[k]
        return pltpu.make_async_copy(gu_any.at[pl.ds(first, units), t], gu.at[t % 2, pl.ds(0, units)], in_sem.at[t % 2])

    def tile_loads(t):
        rows = pl.ds(WIDE * t, WIDE)
        return pltpu.make_async_copy(x_any.at[rows], a0.at[t], tile_sem.at[t, 0]), pltpu.make_async_copy(dh_any.at[t], dh.at[t], tile_sem.at[t, 1])

    for one in (own_load(0), gu_load(0, 0), wd_load, *tile_loads(0), own_load(1)):
        one.start()
    for t in range(1, 4):
        for one in tile_loads(t):
            one.start()
    squares[...] = jnp.zeros_like(squares)

    def c_copy(q):
        return remote(u.at[q, 1 - c], rc.at[q], s1.at[q, 0], r1.at[q, 0], to_core)

    def x_copy(q):
        return remote(sx.at[q], rx.at[q], s1.at[q, 1], r1.at[q, 1], to_x)

    def y_copy(q):
        return remote(sy.at[q], ry.at[q], s1.at[q, 2], r1.at[q, 2], to_y)

    def z_copy(q, k):
        return remote(sz.at[q, k], rz.at[q, k], s3.at[q, 0, k], r3.at[q, 0, k], to_z[k])

    def back_z_copy(q, k):
        return remote(g.at[q, 4 * y + z], g.at[q, 4 * y + z], s3.at[q, 1, k], r3.at[q, 1, k], to_z[k])

    def back_y_copy(q):
        half = g.at[q, pl.ds(4 * y, 4)]
        return remote(half, half, s1.at[q, 3], r1.at[q, 3], to_y)

    def upto_x(q, p):
        return u[q, c, x, p].astype(F32) + rc[q, x, p].astype(F32) + rx[q, p].astype(F32)

    def upto_y(q, k):
        return upto_x(q, 4 * y + k) + ry[q, k].astype(F32)

    def stage0(q):
        c_copy(q).start()

    def stage1(q):
        c_copy(q).wait_recv()
        sx[q] = (u[q, c, 1 - x].astype(F32) + rc[q, 1 - x].astype(F32)).astype(BF)
        x_copy(q).start()

    def stage2(q):
        x_copy(q).wait_recv()
        for k in range(4):
            sy[q, k] = upto_x(q, 4 * (1 - y) + k).astype(BF)
        y_copy(q).start()

    def stage3(q):
        y_copy(q).wait_recv()
        for k in range(3):
            sz[q, k] = upto_y(q, (z + k + 1) % 4).astype(BF)
        for k in range(3):
            z_copy(q, k).start()

    def stage4(q):
        for k in range(3):
            z_copy(q, k).wait_recv()
        total = upto_y(q, z)
        for k in range(3):
            total += rz[q, k].astype(F32)
        g[q, 4 * y + z] = total.astype(BF)
        for k in range(3):
            back_z_copy(q, k).start()

    def stage5(q):
        for k in range(3):
            back_z_copy(q, k).wait_recv()
        back_y_copy(q).start()

    def stage6(q):
        back_y_copy(q).wait_recv()
        wide = g[q].astype(F32).reshape(48, 8, LANE)
        squares[...] += jnp.sum(wide * wide, 0)

    stages = (stage0, stage1, stage2, stage3, stage4, stage5, stage6)

    def tick(m):
        for j in reversed(range(7)):
            q = m - max(2 * j - 1, 0)

            @pl.when((q >= 0) & (q < ALL))
            def _():
                stages[j](q)

    own_load(0).wait()
    greeted()
    tick(0)
    wd_load.wait()
    for number, (first, units) in enumerate(CHUNKS):
        acc_d[...] = jnp.zeros_like(acc_d)
        acc_gu[...] = jnp.zeros_like(acc_gu)

        @pl.loop(0, 4)
        def _(t):
            @pl.when(t < 3)
            def _():
                gu_load(number, t + 1).start()

            if number < 3:

                @pl.when(t == 3)
                def _():
                    gu_load(number + 1, 0).start()

            gu_load(number, t).wait()
            if number == 0:
                for one in tile_loads(t):
                    one.wait()
                wide = a0[t].astype(F32)
                a0[t] = (wide * lax.rsqrt(jnp.mean(wide * wide, -1, keepdims=True) + 1e-6)).astype(BF)
            a, h = a0[t], dh[t]
            for n in range(units):
                d = nn(wd[first + n].reshape(LANE, D), h).astype(BF).astype(F32)
                one, dg, du = backward_unit(gu[t % 2, n, :LANE, :], gu[t % 2, n, LANE:, :], d)
                act[LANE * n : LANE * n + LANE, :] = one
                dgu[PAIR * n : PAIR * n + LANE, :] = dg
                dgu[PAIR * n + LANE : PAIR * n + PAIR, :] = du
            acc_d[: LANE * units, :] += nt(act[: LANE * units, :], h)
            acc_gu[: PAIR * units, :] += nn(dgu[: PAIR * units, :], a)

            if number == 0:

                @pl.when(t == 0)
                def _():
                    own_load(1).wait()

            tick(5 * number + t + 1)

        @pl.loop(0, units)
        def _(n):
            pack(UNITS + first + n, acc_gu, acc_d, n, u)

        tick(5 * number + 5)

    @pl.loop(21, ALL + 11)
    def _(m):
        tick(m)

    mine = sums.at[2 * x + c]
    norm = [remote(mine, mine, norm_send.at[k], norm_recv.at[k], group[k]) for k in range(3)]
    sums[2 * x + c] = squares[...]
    for one in norm:
        one.start()
    g_out[...] = g[...]

    @pl.loop(0, ALL)
    def _(q):
        for one in (c_copy(q), x_copy(q), y_copy(q), back_y_copy(q)):
            one.wait_send()
        for k in range(3):
            z_copy(q, k).wait_send()
            back_z_copy(q, k).wait_send()

    for one in norm:
        one.wait()
    total_out[...] = sums[0] + sums[1] + sums[2] + sums[3]


def third_kernel(g_ref, total_ref, *refs):
    weights, ms, vs = refs[0:3], refs[3:6], refs[6:9]
    outs, buffers = refs[9:18], refs[18:27]
    turned, plain, sem = refs[27:30]
    factor = jnp.minimum(1.0, 0.5 * lax.rsqrt(jnp.sum(total_ref[...]) / COUNT + 1e-30))

    def copies(l, i):
        return [pltpu.make_async_copy(buffers[k].at[l], outs[k].at[l], sem.at[l, k]) for k in (i, 3 + i, 6 + i)]

    def take(l, i, g):
        g = g * factor
        m = 0.9 * ms[i][l] + 0.1 * g
        v = 0.95 * vs[i][l] + 0.05 * g * g
        w = weights[i][l].astype(F32)
        buffers[3 + i][l] = m
        buffers[6 + i][l] = v
        buffers[i][l] = (w - 0.02 * (m * lax.rsqrt(v + 1e-8) + 0.1 * w)).astype(BF)
        for one in copies(l, i):
            one.start()

    for l in range(2):
        for n in range(UNITS):
            for p in range(8):
                row = SEG * n + 16 * (p // 4)
                plain[row : row + 16, LANE * (p % 4) : LANE * (p % 4) + LANE] = g_ref[1 - l, n, p, 32:48, :].astype(F32)
        take(l, 2, plain[...])
        for i in range(2):
            for n in range(UNITS):
                for s in range(4):
                    turned[352 * s + SEG * n : 352 * s + SEG * n + SEG, :] = g_ref[1 - l, n, 4 * i + s, 0:32, :].astype(F32)
            take(l, i, turned[...].T)
    for l in range(2):
        for i in range(3):
            for one in copies(l, i):
                one.wait()


def step(x, dy, w_gate, w_up, w_down, *moments):
    tokens = x.shape[1]
    tiles = tokens // TT
    any_ = pl.BlockSpec(memory_space=pl.ANY)

    def once(shape):
        return pl.BlockSpec(shape, lambda i: (0,) * len(shape), pipeline_mode=pl.Buffered(1))

    unit = (UNITS, 2, 2, 8, 48, LANE)
    dma = pltpu.SemaphoreType.DMA
    u1, dh, gu0, wd0 = pl.pallas_call(
        first_kernel,
        grid=(2 + tiles,),
        in_specs=[
            pl.BlockSpec((tiles // 2, TT, D), lambda i: (jnp.minimum(i, 1), 0, 0)),
            pl.BlockSpec((TT, D), lambda i: (jnp.maximum(i - 2, 0), 0)),
            once(w_gate.shape), once(w_up.shape), once(w_down.shape),
        ],
        out_specs=[any_, pl.BlockSpec((1, D, TT), lambda i: (jnp.maximum(i - 2, 0) // 2, 0, jnp.maximum(i - 2, 0) % 2)), any_, any_],
        out_shape=[
            jax.ShapeDtypeStruct(unit, BF),
            jax.ShapeDtypeStruct((tiles // 2, D, WIDE), BF),
            jax.ShapeDtypeStruct((UNITS, tiles // 2, PAIR, WIDE), F32),
            jax.ShapeDtypeStruct((2, UNITS, 4, SEG, D), BF),
        ],
        scratch_shapes=[
            pltpu.VMEM(unit, BF),
            pltpu.VMEM((2, UNITS, 2, LANE, D), BF),
            pltpu.VMEM((2, UNITS, 4, SEG, D), BF),
            pltpu.VMEM((tiles, D, TT), BF),
            pltpu.VMEM((tiles // 2, FF, TT), BF),
            pltpu.VMEM((tiles // 2, TT, D), BF),
            pltpu.VMEM((2, UNITS, PAIR, TT), F32),
            pltpu.VMEM((2 * FF, TT), BF),
            pltpu.VMEM((D, FF), BF),
            pltpu.VMEM((2 * FF, D), F32),
            pltpu.VMEM((FF, D), F32),
            dma((2, 2)), dma((2, 2)), dma((2, 5, 4)), dma((2, 5, 4)), dma((4, 2)), dma((UNITS,)), dma((1,)),
        ],
        compiler_params=pltpu.CompilerParams(vmem_limit_bytes=VMEM_LIMIT, collective_id=0, has_side_effects=True),
        name="gather_forward_and_last_layer",
    )(x.reshape(tiles, TT, D), dy[0], w_gate, w_up, w_down)

    most = max(units for _, units in CHUNKS)
    g, total = pl.pallas_call(
        second_kernel,
        in_specs=[pl.BlockSpec(memory_space=pltpu.HBM)] * 5,
        out_specs=[pl.BlockSpec(memory_space=pltpu.VMEM)] * 2,
        out_shape=[jax.ShapeDtypeStruct((ALL, 8, 48, LANE), BF), jax.ShapeDtypeStruct((8, LANE), F32)],
        scratch_shapes=[
            pltpu.VMEM((tiles // 2, WIDE, D), BF),
            pltpu.VMEM((tiles // 2, D, WIDE), BF),
            pltpu.VMEM((2, most, PAIR, WIDE), F32),
            pltpu.VMEM((UNITS, 4, SEG, D), BF),
            pltpu.VMEM((ALL, 2, 2, 8, 48, LANE), BF),
            pltpu.VMEM((LANE * most, WIDE), BF),
            pltpu.VMEM((PAIR * most, WIDE), BF),
            pltpu.VMEM((PAIR * most, D), F32),
            pltpu.VMEM((LANE * most, D), F32),
            pltpu.VMEM((ALL, 2, 8, 48, LANE), BF),
            pltpu.VMEM((ALL, 8, 48, LANE), BF),
            pltpu.VMEM((ALL, 8, 48, LANE), BF),
            pltpu.VMEM((ALL, 4, 48, LANE), BF),
            pltpu.VMEM((ALL, 4, 48, LANE), BF),
            pltpu.VMEM((ALL, 3, 48, LANE), BF),
            pltpu.VMEM((ALL, 3, 48, LANE), BF),
            pltpu.VMEM((ALL, 8, 48, LANE), BF),
            pltpu.VMEM((4, 8, LANE), F32),
            pltpu.VMEM((8, LANE), F32),
            dma((ALL, 4)), dma((ALL, 4)), dma((ALL, 2, 3)), dma((ALL, 2, 3)),
            dma((3,)), dma((3,)), dma((5,)), dma((tiles, 2)),
        ],
        compiler_params=pltpu.CompilerParams(vmem_limit_bytes=50 * MIB, collective_id=1, has_side_effects=True),
        name="first_layer_and_sums",
    )(x[0], dh, gu0, wd0, u1)

    arrays = (w_gate, w_up, w_down, *moments)

    vmem = pl.BlockSpec(memory_space=pltpu.VMEM)
    return pl.pallas_call(
        third_kernel,
        in_specs=[vmem] * (2 + len(arrays)),
        out_specs=[any_] * len(arrays),
        out_shape=[jax.ShapeDtypeStruct(a.shape, a.dtype) for a in arrays],
        scratch_shapes=[pltpu.VMEM(a.shape, a.dtype) for a in arrays]
        + [pltpu.VMEM((FF, LANE), F32), pltpu.VMEM((FF // 4, D), F32), dma((2, 9))],
        compiler_params=pltpu.CompilerParams(vmem_limit_bytes=28 * MIB),
        name="clip_and_adamw",
    )(g.reshape(2, UNITS, 8, 48, LANE), total, *arrays)


def solution(mesh):
    states, cut = P(("rep", "r", "s"), None, None), P(None, "s", None)
    return jax.shard_map(
        lambda *arrays: tuple(step(*arrays)),
        mesh=mesh,
        in_specs=(states, states) + (cut,) * 9,
        out_specs=(P("rep", "s", None),) * 9,
        check_vma=False,
    )
```
